128 devices in a mesh: cells: 32 (over y, x, core), vecs: 4 (over z).
Axes of the slice: x: 4, y: 4, z: 4, core: 2. Of those that a mesh axis runs over, the one named last changes fastest.
Arguments:
- vectors: float32 [64, 32, 64, 128], P(None, 'cells', 'vecs'), may hold values from -120 to 120
- potential: float32 [64, 32, 128], P(None, 'cells'), may hold values from -0.5 to 0.5
- hopping: float32 [27, 64, 64], replicated, may hold values from -0.07 to 0.07
- center: float32 [1], replicated, may hold values from -0.3 to 0.3
Outputs:
- filtered: float32 [64, 32, 64, 128], P(None, 'cells', 'vecs')
The draws below stay inside these ranges and needn't reach their ends.
All inputs are finite; a program needn't handle non-finite values.
Results may differ from the reference program's by a relative error of at most 0.0003.
Values sent between devices are 32-bit elements; how exact they have to be, the bound alone decides.
No kernel may reach another device: no remote copies, remote signals or barrier semaphores. Data moves between devices by JAX's collectives and lax.ppermute only.
A program may use at most 128 MiB of HBM per device.

```python
import math
import jax
import jax.numpy as jnp
from jax import lax

ORB = 64
NVEC = 64
NY = 16
STEPS = 4
NX = 32
NZ = 8


def draw_vectors(key, part):
    base_key, spread_key, weight_key = jax.random.split(jax.random.fold_in(key, 11), 3)
    base = jax.random.truncated_normal(base_key, -4.0, 4.0, (ORB, NX, NVEC, NY * NZ), jnp.float32)
    common = 0.5
    spread = jax.random.truncated_normal(spread_key, -4.0, 4.0, (NVEC, NVEC), jnp.float32)
    weights = jax.random.uniform(weight_key, (NVEC,), jnp.float32, -1.0, 1.0)
    scale = 1.0 / math.sqrt(NVEC)
    mixer = jnp.eye(NVEC, dtype=jnp.float32) + 0.7 * scale * spread
    mixer = mixer + common * scale * jnp.ones((NVEC, 1), jnp.float32) * weights[None, :]
    return jnp.einsum('oxkc,ku->oxuc', base, mixer)


def levels(key, shape, cuts, least, largest):
    loudness = 1.0
    for axis_at, parts in cuts:
        steps = jax.random.uniform(jax.random.fold_in(jax.random.fold_in(key, 6), axis_at), (parts,), jnp.float32, least / len(cuts), largest / len(cuts))
        loudness = loudness * jnp.repeat(jnp.exp(steps), shape[axis_at] // parts).reshape((-1,) + (1,) * (len(shape) - 1 - axis_at))
    return loudness


def scatter_about(own_key, dims, deviation, most, held_as=jnp.bfloat16):
    array = deviation * jax.random.normal(own_key, dims, jnp.float32)
    return jnp.clip(array, min=-most, max=most).astype(held_as)


def setup_inputs(seed: int = 0) -> dict:
    key_of = jax.random.split(jax.random.key(seed), 5)
    return {
        "vectors": draw_vectors(jax.random.fold_in(key_of[4], 71), 0),
        "potential": jnp.clip(jax.random.uniform(key_of[1], (ORB, NX, NY * NZ), jnp.float32, -0.5, 0.5) * levels(key_of[1], (ORB, NX, NY * NZ), ((1, 32),), -0.4, 0.0), -0.5, 0.5),
        "hopping": scatter_about(key_of[2], (27, ORB, ORB), 0.012, 0.07, jnp.float32),
        "center": jnp.clip(jax.random.uniform(key_of[3], (1,), jnp.float32, -0.3, 0.3), -0.3, 0.3),
    }


HIGH = lax.Precision.HIGHEST

def symmetric_blocks(hopping):
    return 0.5 * (hopping + jnp.transpose(hopping[::-1], (0, 2, 1)))

def apply_lattice(field_in, potential, center, blocks):
    orbits, width_x, bundle, merged = field_in.shape

    def one_slice(index):
        onsite = lax.dynamic_index_in_dim(potential, index, 1, keepdims=False) - center[0]
        own = lax.dynamic_index_in_dim(field_in, index, 1, keepdims=False)
        running = onsite[:, None, :] * own
        for offset in range(3):
            where = (index + offset - 1 + width_x) % width_x
            source = lax.dynamic_index_in_dim(field_in, where, 1, keepdims=False)
            stacked = blocks[9 * offset:9 * offset + 9].reshape(9 * orbits, orbits)
            product = jnp.dot(stacked, source.reshape(orbits, -1), precision=HIGH, preferred_element_type=jnp.float32)
            product = product.reshape(9, orbits, bundle, NY, NZ)
            for inner in range(9):
                moved = jnp.roll(product[inner], (1 - inner // 3, 1 - inner % 3), axis=(2, 3))
                running = running + moved.reshape(orbits, bundle, merged)
        return running
    slices = lax.map(one_slice, jnp.arange(width_x, dtype=jnp.int32))
    return jnp.moveaxis(slices, 0, 1)

def reference(vectors, potential, hopping, center):
    blocks = symmetric_blocks(hopping)
    previous = vectors
    current = apply_lattice(vectors, potential, center, blocks)
    for step in range(STEPS - 1):
        following = 2.0 * apply_lattice(current, potential, center, blocks) - previous
        previous, current = (current, following)
    gram_matrix = lax.dot_general(current, current, (((0, 1, 3), (0, 1, 3)), ((), ())), precision=HIGH, preferred_element_type=jnp.float32)
    frobenius = jnp.sqrt(jnp.sum(gram_matrix * gram_matrix))
    mixing = (1.5 * jnp.eye(NVEC, dtype=jnp.float32) - 0.5 * gram_matrix / frobenius) / jnp.sqrt(frobenius)
    result = jnp.einsum('oxuc,uv->oxvc', current, mixing, precision=HIGH)
    return result * jnp.sqrt(jnp.float32(NX * NY * NZ))
```

```python
import math

import jax
import jax.numpy as jnp
from jax import lax
from jax.experimental import pallas as pl
from jax.experimental.pallas import tpu as pltpu
from jax.sharding import Mesh, PartitionSpec as P

ORB = 64
NVEC = 64
NY = 16
NZ = 8
CELLS = NY * NZ
STEPS = 4
HALF = 8
F32 = jnp.float32
BF16 = jnp.bfloat16


def split(x):
    high = x.astype(BF16)
    return high, (x - high.astype(F32)).astype(BF16)


def weights_body(hop, out):
    for iz in range(3):
        for iy in range(3):
            parts = []
            for ix in range(3):
                d = 9 * ix + 3 * iy + iz
                parts.append(0.5 * (hop[d] + jnp.transpose(hop[26 - d])))
            row = jnp.concatenate(parts, axis=1)
            high, low = split(row)
            high = high.astype(F32)
            whole = jnp.concatenate([high, high, low.astype(F32)], axis=1)
            at = (3 * iz + iy) * ORB
            out[at : at + ORB, :] = whole.astype(BF16)


def weights(hopping):
    return pl.pallas_call(
        weights_body,
        out_shape=jax.ShapeDtypeStruct((9 * ORB, 9 * ORB), BF16),
    )(hopping)


def step_body(first, *refs):
    if first:
        center, pot, w, cur, left, right, out = refs
    else:
        center, pot, w, cur, left, right, prev, out = refs
    onsite = pot[...] - center[0]
    lane = lax.broadcasted_iota(jnp.int32, (ORB, CELLS), 1) % NZ
    for pair in range(HALF // 2):
        rows = [pl.ds(2 * pair + i, ORB, stride=HALF) for i in range(2)]
        own = [cur[r, :] for r in rows]
        planes = jnp.concatenate(
            [
                jnp.concatenate([left[rows[i], :], own[i], right[rows[i], :]], axis=0)
                for i in range(2)
            ],
            axis=1,
        )
        high, low = split(planes)
        stacked = jnp.concatenate([high, low, high], axis=0)
        product = jnp.dot(w[...], stacked, preferred_element_type=F32)
        for i in range(2):
            mine = product[:, i * CELLS : (i + 1) * CELLS]
            total = onsite * own[i]
            for iz in range(3):
                below, here, above = (
                    mine[(3 * iz + iy) * ORB : (3 * iz + iy + 1) * ORB] for iy in range(3)
                )
                t = here + pltpu.roll(below, NZ, 1) + pltpu.roll(above, CELLS - NZ, 1)
                if iz == 0:
                    t = jnp.where(lane == 0, pltpu.roll(t, CELLS - NZ + 1, 1), pltpu.roll(t, 1, 1))
                elif iz == 2:
                    t = jnp.where(
                        lane == NZ - 1, pltpu.roll(t, NZ - 1, 1), pltpu.roll(t, CELLS - 1, 1)
                    )
                total = total + t
            if not first:
                total = 2.0 * total - prev[rows[i], :]
            out[rows[i], :] = total


def apply_step(center, pot, w, cur, left, right, prev=None):
    first = prev is None
    vmem = pl.BlockSpec(memory_space=pltpu.VMEM)
    args = (center, pot, w, cur, left, right) + (() if first else (prev,))
    return pl.pallas_call(
        lambda *refs: step_body(first, *refs),
        in_specs=[pl.BlockSpec(memory_space=pltpu.SMEM)] + [vmem] * (len(args) - 1),
        out_specs=vmem,
        out_shape=jax.ShapeDtypeStruct((ORB * HALF, CELLS), F32),
    )(*args)


def gram_body(*refs):
    pieces, out = refs[:-1], refs[-1]
    total = jnp.zeros((NVEC, 2 * NVEC), F32)
    for o in range(0, ORB, 2):
        rows = jnp.concatenate(
            [
                jnp.concatenate([p[(o + i) * HALF : (o + i + 1) * HALF, :] for p in pieces], axis=0)
                for i in range(2)
            ],
            axis=1,
        )
        high, low = split(rows)
        both = jnp.concatenate([high, low], axis=0)
        total = total + lax.dot_general(
            high, both, (((1,), (1,)), ((), ())), preferred_element_type=F32
        )
    cross = total[:, NVEC:]
    gram = total[:, :NVEC] + cross + jnp.transpose(cross)
    out[...] = jnp.concatenate([gram[: NVEC // 2], gram[NVEC // 2 :]], axis=1)


def gram_of(pieces):
    return pl.pallas_call(
        gram_body, out_shape=jax.ShapeDtypeStruct((NVEC // 2, 2 * NVEC), F32)
    )(*pieces)


def mix_body(factor, copies, *refs):
    pieces, out = refs[:-1], refs[-1]
    packed = jnp.sum(copies[...], axis=0)
    gram = jnp.concatenate([packed[:, :NVEC], packed[:, NVEC:]], axis=0)
    squares = jnp.sum(jnp.sum(gram * gram, axis=1, keepdims=True), axis=0, keepdims=True)
    frobenius = jnp.sqrt(squares)
    mine = gram[: 2 * HALF]
    rows = lax.broadcasted_iota(jnp.int32, mine.shape, 0)
    cols = lax.broadcasted_iota(jnp.int32, mine.shape, 1)
    eye = jnp.where(rows == cols, 1.0, 0.0).astype(F32)
    mixing = (1.5 * eye - 0.5 * mine / frobenius) * (factor / jnp.sqrt(frobenius))
    tall = jnp.concatenate([mixing] * 4, axis=0)
    wide = jnp.concatenate([tall] * 4, axis=1)
    rows = lax.broadcasted_iota(jnp.int32, wide.shape, 0) // (2 * HALF)
    cols = lax.broadcasted_iota(jnp.int32, wide.shape, 1) // NVEC
    wide = jnp.where(rows == cols, wide, 0.0)
    high, low = split(wide)
    lhs = jnp.concatenate([high, high, low], axis=1)
    for group in range(ORB // 8):
        halves = []
        for side in range(2):
            at = group * 8 + side * 4
            halves.append(
                jnp.concatenate(
                    [
                        p[(at + i) * HALF : (at + i + 1) * HALF, :]
                        for i in range(4)
                        for p in pieces
                    ],
                    axis=0,
                )
            )
        data = jnp.concatenate(halves, axis=1)
        high, low = split(data)
        rhs = jnp.concatenate([high, low, high], axis=0)
        mixed = jnp.dot(lhs, rhs, preferred_element_type=F32)
        for side in range(2):
            at = (group * 8 + side * 4) * 2 * HALF
            out[at : at + 8 * HALF, :] = mixed[:, side * CELLS : (side + 1) * CELLS]


def mix(factor, copies, pieces):
    return pl.pallas_call(
        lambda *refs: mix_body(factor, *refs),
        out_shape=jax.ShapeDtypeStruct((ORB * 2 * HALF, CELLS), F32),
    )(copies, *pieces)


def shards(vectors, potential, hopping, center):
    cells = ("chip", "core")
    count = lax.axis_size("chip") * lax.axis_size("core")
    ring = lax.axis_size("vecs")
    up = [(i, (i + 1) % count) for i in range(count)]
    down = [(j, i) for i, j in up]
    zup = [(i, (i + 1) % ring) for i in range(ring)]
    zdown = [(j, i) for i, j in zup]
    pot = potential.reshape(ORB, CELLS)
    halves = [
        vectors[:, 0, h * HALF : (h + 1) * HALF].reshape(ORB * HALF, CELLS) for h in range(2)
    ]
    w = weights(hopping)
    prev = [None, None]
    cur = halves
    for step in range(STEPS):
        following = []
        for h in range(2):
            left = lax.ppermute(cur[h], cells, up)
            right = lax.ppermute(cur[h], cells, down)
            following.append(apply_step(center, pot, w, cur[h], left, right, prev[h]))
        prev, cur = cur, following
    a, b = cur
    a_below = lax.ppermute(a, "vecs", zup)
    a_above = lax.ppermute(a, "vecs", zdown)
    a_far = lax.ppermute(a_below, "vecs", zup)
    b_below = lax.ppermute(b, "vecs", zup)
    b_above = lax.ppermute(b, "vecs", zdown)
    b_far = lax.ppermute(b_above, "vecs", zdown)
    pieces = (a, b, a_above, b_above, a_far, b_far, a_below, b_below)
    gram = gram_of(pieces)
    gram = gram + lax.ppermute(gram, "core", [(0, 1), (1, 0)])
    chips = lax.axis_size("chip")
    copies = lax.all_to_all(
        jnp.broadcast_to(gram, (chips, *gram.shape)), "chip", split_axis=0, concat_axis=0, tiled=True
    )
    factor = math.sqrt(float(count * CELLS))
    out = mix(factor, copies, pieces)
    return out.reshape(ORB, 1, 2 * HALF, CELLS)


def solution(mesh):
    cells, vecs = mesh.shape["cells"], mesh.shape["vecs"]
    fine = Mesh(mesh.devices.reshape(cells // 2, 2, vecs), ("chip", "core", "vecs"))
    both = ("chip", "core")
    placed = (P(None, both, "vecs", None), P(None, both, None), P(), P())
    return jax.shard_map(
        shards,
        mesh=fine,
        in_specs=placed,
        out_specs=P(None, both, "vecs", None),
        check_vma=False,
    )
```

```python
import math

import jax
import jax.numpy as jnp
from jax import lax
from jax.experimental import pallas as pl
from jax.experimental.pallas import tpu as pltpu
from jax.sharding import Mesh, PartitionSpec as P

ORB = 64
NVEC = 64
NY = 16
NZ = 8
CELLS = NY * NZ
STEPS = 4
HALF = 8
F32 = jnp.float32
BF16 = jnp.bfloat16


LIMIT = pltpu.CompilerParams(vmem_limit_bytes=8 * 1024 * 1024)


def split(x):
    high = x.astype(BF16)
    return high, (x - high.astype(F32)).astype(BF16)


def weights_body(order, hop, out):
    for iz in range(3):
        for iy in range(3):
            parts = []
            for ix in range(3):
                d = 9 * order[ix] + 3 * iy + iz
                parts.append(0.5 * (hop[d] + jnp.transpose(hop[26 - d])))
            row = jnp.concatenate(parts, axis=1)
            high, low = split(row)
            high = high.astype(F32)
            whole = jnp.concatenate([high, high, low.astype(F32)], axis=1)
            at = (3 * iz + iy) * ORB
            out[at : at + ORB, :] = whole.astype(BF16)


def weights(order, hopping):
    return pl.pallas_call(
        weights_body,
        in_specs=[pl.BlockSpec(memory_space=pltpu.SMEM), pl.BlockSpec(memory_space=pltpu.VMEM)],
        out_shape=jax.ShapeDtypeStruct((9 * ORB, 9 * ORB), BF16),
        compiler_params=LIMIT,
    )(order, hopping)


def step_body(first, *refs):
    if first:
        center, pot, w, cur, left, right, out = refs
    else:
        center, pot, w, cur, left, right, prev, out = refs
    onsite = pot[...] - center[0]
    lane = lax.broadcasted_iota(jnp.int32, (ORB, CELLS), 1) % NZ
    for pair in range(HALF // 2):
        rows = [pl.ds(2 * pair + i, ORB, stride=HALF) for i in range(2)]
        own = [cur[r, :] for r in rows]
        planes = jnp.concatenate(
            [
                jnp.concatenate([left[rows[i], :], own[i], right[rows[i], :]], axis=0)
                for i in range(2)
            ],
            axis=1,
        )
        high, low = split(planes)
        stacked = jnp.concatenate([high, low, high], axis=0)
        product = jnp.dot(w[...], stacked, preferred_element_type=F32)
        for i in range(2):
            mine = product[:, i * CELLS : (i + 1) * CELLS]
            total = onsite * own[i]
            for iz in range(3):
                below, here, above = (
                    mine[(3 * iz + iy) * ORB : (3 * iz + iy + 1) * ORB] for iy in range(3)
                )
                t = here + pltpu.roll(below, NZ, 1) + pltpu.roll(above, CELLS - NZ, 1)
                if iz == 0:
                    t = jnp.where(lane == 0, pltpu.roll(t, CELLS - NZ + 1, 1), pltpu.roll(t, 1, 1))
                elif iz == 2:
                    t = jnp.where(
                        lane == NZ - 1, pltpu.roll(t, NZ - 1, 1), pltpu.roll(t, CELLS - 1, 1)
                    )
                total = total + t
            if not first:
                total = 2.0 * total - prev[rows[i], :]
            out[rows[i], :] = total


def apply_step(center, pot, w, cur, left, right, prev=None):
    first = prev is None
    vmem = pl.BlockSpec(memory_space=pltpu.VMEM)
    args = (center, pot, w, cur, left, right) + (() if first else (prev,))
    return pl.pallas_call(
        lambda *refs: step_body(first, *refs),
        in_specs=[pl.BlockSpec(memory_space=pltpu.SMEM)] + [vmem] * (len(args) - 1),
        out_specs=vmem,
        out_shape=jax.ShapeDtypeStruct((ORB * HALF, CELLS), F32),
        compiler_params=LIMIT,
    )(*args)


def gram_body(*refs):
    pieces, out = refs[:-1], refs[-1]
    total = jnp.zeros((NVEC, 2 * NVEC), F32)
    for o in range(0, ORB, 2):
        rows = jnp.concatenate(
            [
                jnp.concatenate([p[(o + i) * HALF : (o + i + 1) * HALF, :] for p in pieces], axis=0)
                for i in range(2)
            ],
            axis=1,
        )
        high, low = split(rows)
        both = jnp.concatenate([high, low], axis=0)
        total = total + lax.dot_general(
            high, both, (((1,), (1,)), ((), ())), preferred_element_type=F32
        )
    cross = total[:, NVEC:]
    gram = total[:, :NVEC] + cross + jnp.transpose(cross)
    out[...] = jnp.concatenate([gram[: NVEC // 2], gram[NVEC // 2 :]], axis=1)


def gram_of(pieces):
    return pl.pallas_call(
        gram_body,
        out_shape=jax.ShapeDtypeStruct((NVEC // 2, 2 * NVEC), F32),
        compiler_params=LIMIT,
    )(*pieces)


def mix_body(factor, copies, *refs):
    pieces, out = refs[:-1], refs[-1]
    packed = jnp.sum(copies[...], axis=0)
    gram = jnp.concatenate([packed[:, :NVEC], packed[:, NVEC:]], axis=0)
    squares = jnp.sum(jnp.sum(gram * gram, axis=1, keepdims=True), axis=0, keepdims=True)
    frobenius = jnp.sqrt(squares)
    mine = gram[: 2 * HALF]
    rows = lax.broadcasted_iota(jnp.int32, mine.shape, 0)
    cols = lax.broadcasted_iota(jnp.int32, mine.shape, 1)
    eye = jnp.where(rows == cols, 1.0, 0.0).astype(F32)
    mixing = (1.5 * eye - 0.5 * mine / frobenius) * (factor / jnp.sqrt(frobenius))
    tall = jnp.concatenate([mixing] * 4, axis=0)
    wide = jnp.concatenate([tall] * 4, axis=1)
    rows = lax.broadcasted_iota(jnp.int32, wide.shape, 0) // (2 * HALF)
    cols = lax.broadcasted_iota(jnp.int32, wide.shape, 1) // NVEC
    wide = jnp.where(rows == cols, wide, 0.0)
    high, low = split(wide)
    lhs = jnp.concatenate([high, high, low], axis=1)
    for group in range(ORB // 8):
        halves = []
        for side in range(2):
            at = group * 8 + side * 4
            halves.append(
                jnp.concatenate(
                    [
                        p[(at + i) * HALF : (at + i + 1) * HALF, :]
                        for i in range(4)
                        for p in pieces
                    ],
                    axis=0,
                )
            )
        data = jnp.concatenate(halves, axis=1)
        high, low = split(data)
        rhs = jnp.concatenate([high, low, high], axis=0)
        mixed = jnp.dot(lhs, rhs, preferred_element_type=F32)
        for side in range(2):
            at = (group * 8 + side * 4) * 2 * HALF
            out[at : at + 8 * HALF, :] = mixed[:, side * CELLS : (side + 1) * CELLS]


def mix(factor, copies, pieces):
    return pl.pallas_call(
        lambda *refs: mix_body(factor, *refs),
        out_shape=jax.ShapeDtypeStruct((ORB * 2 * HALF, CELLS), F32),
        compiler_params=LIMIT,
    )(copies, *pieces)


def shards(vectors, potential, hopping, center):
    cells = ("chip", "core")
    count = lax.axis_size("chip") * lax.axis_size("core")
    ring = lax.axis_size("vecs")
    outer = [(i, (i + 1) % count if i % 2 else (i - 1) % count) for i in range(count)]
    inner = [(0, 1), (1, 0)]
    near = [(i, i ^ 1) for i in range(ring)]
    other = [(i, i ^ 3) for i in range(ring)]
    pot = potential.reshape(ORB, CELLS)
    halves = [
        vectors[:, 0, h * HALF : (h + 1) * HALF].reshape(ORB * HALF, CELLS) for h in range(2)
    ]
    core = lax.axis_index("core")
    order = jnp.stack([2 * core, jnp.ones_like(core), 2 - 2 * core]).astype(jnp.int32)
    w = weights(order, hopping)
    prev = [None, None]
    cur = halves
    for step in range(STEPS):
        following = []
        for h in range(2):
            away = lax.ppermute(cur[h], cells, outer)
            beside = lax.ppermute(cur[h], "core", inner)
            following.append(apply_step(center, pot, w, cur[h], away, beside, prev[h]))
        prev, cur = cur, following
    a, b = cur
    a_near = lax.ppermute(a, "vecs", near)
    a_other = lax.ppermute(a, "vecs", other)
    a_far = lax.ppermute(a_other, "vecs", near)
    b_near = lax.ppermute(b, "vecs", near)
    b_other = lax.ppermute(b, "vecs", other)
    b_far = lax.ppermute(b_near, "vecs", other)
    pieces = (a, b, a_near, b_near, a_far, b_far, a_other, b_other)
    gram = gram_of(pieces)
    gram = gram + lax.ppermute(gram, "core", [(0, 1), (1, 0)])
    chips = lax.axis_size("chip")
    copies = lax.all_to_all(
        jnp.broadcast_to(gram, (chips, *gram.shape)), "chip", split_axis=0, concat_axis=0, tiled=True
    )
    factor = math.sqrt(float(count * CELLS))
    out = mix(factor, copies, pieces)
    return out.reshape(ORB, 1, 2 * HALF, CELLS)


def solution(mesh):
    cells, vecs = mesh.shape["cells"], mesh.shape["vecs"]
    fine = Mesh(mesh.devices.reshape(cells // 2, 2, vecs), ("chip", "core", "vecs"))
    both = ("chip", "core")
    placed = (P(None, both, "vecs", None), P(None, both, None), P(), P())
    return jax.shard_map(
        shards,
        mesh=fine,
        in_specs=placed,
        out_specs=P(None, both, "vecs", None),
        check_vma=False,
    )
```

```python
import math

import jax
import jax.numpy as jnp
from jax import lax
from jax.experimental import pallas as pl
from jax.experimental.pallas import tpu as pltpu
from jax.sharding import Mesh, PartitionSpec as P

ORB = 64
NVEC = 64
NY = 16
NZ = 8
CELLS = NY * NZ
STEPS = 4
HALF = 8
F32 = jnp.float32
BF16 = jnp.bfloat16


LIMIT = pltpu.CompilerParams(vmem_limit_bytes=8 * 1024 * 1024)


def split(x):
    high = x.astype(BF16)
    return high, (x - high.astype(F32)).astype(BF16)


def halves_body(vectors, *refs):
    copies = [
        pltpu.make_async_copy(vectors.at[:, h * HALF : (h + 1) * HALF], refs[h], refs[2 + h])
        for h in range(2)
    ]
    for copy in copies:
        copy.start()
    for copy in copies:
        copy.wait()


def split_halves(vectors):
    vmem = pl.BlockSpec(memory_space=pltpu.VMEM)
    return pl.pallas_call(
        halves_body,
        in_specs=[pl.BlockSpec(memory_space=pl.ANY)],
        out_specs=[vmem, vmem],
        out_shape=[jax.ShapeDtypeStruct((ORB, HALF, CELLS), F32)] * 2,
        scratch_shapes=[pltpu.SemaphoreType.DMA, pltpu.SemaphoreType.DMA],
        compiler_params=LIMIT,
    )(vectors)


def weights_body(order, hop, out):
    for iz in range(3):
        parts = []
        for iy in range(3):
            for ix in range(3):
                d = 9 * order[ix] + 3 * iy + iz
                parts.append(0.5 * (hop[d] + jnp.transpose(hop[26 - d])))
        high, low = split(jnp.concatenate(parts, axis=1))
        high = high.astype(F32)
        whole = jnp.concatenate([high, high, low.astype(F32)], axis=1)
        out[iz * ORB : (iz + 1) * ORB, :] = whole.astype(BF16)


def weights(order, hopping):
    return pl.pallas_call(
        weights_body,
        in_specs=[pl.BlockSpec(memory_space=pltpu.SMEM), pl.BlockSpec(memory_space=pltpu.VMEM)],
        out_shape=jax.ShapeDtypeStruct((3 * ORB, 27 * ORB), BF16),
        compiler_params=LIMIT,
    )(order, hopping)


def step_body(first, *refs):
    if first:
        center, pot, w, cur, left, right, out = refs
    else:
        center, pot, w, cur, left, right, prev, out = refs
    onsite = pot[...] - center[0]
    lane = lax.broadcasted_iota(jnp.int32, (ORB, CELLS), 1) % NZ
    for pair in range(HALF // 2):
        rows = [pl.ds(2 * pair + i, ORB, stride=HALF) for i in range(2)]
        own = [cur[r, :] for r in rows]
        columns = []
        for i in range(2):
            here = jnp.concatenate([left[rows[i], :], own[i], right[rows[i], :]], axis=0)
            below, above = pltpu.roll(here, NZ, 1), pltpu.roll(here, CELLS - NZ, 1)
            columns.append(jnp.concatenate([below, here, above], axis=0))
        high, low = split(jnp.concatenate(columns, axis=1))
        stacked = jnp.concatenate([high, low, high], axis=0)
        product = jnp.dot(w[...], stacked, preferred_element_type=F32)
        for i in range(2):
            below, here, above = (
                product[iz * ORB : (iz + 1) * ORB, i * CELLS : (i + 1) * CELLS] for iz in range(3)
            )
            below = jnp.where(
                lane == 0, pltpu.roll(below, CELLS - NZ + 1, 1), pltpu.roll(below, 1, 1)
            )
            above = jnp.where(
                lane == NZ - 1, pltpu.roll(above, NZ - 1, 1), pltpu.roll(above, CELLS - 1, 1)
            )
            total = onsite * own[i] + here + below + above
            if not first:
                total = 2.0 * total - prev[rows[i], :]
            out[rows[i], :] = total


def apply_step(center, pot, w, cur, left, right, prev=None):
    first = prev is None
    vmem = pl.BlockSpec(memory_space=pltpu.VMEM)
    args = (center, pot, w, cur, left, right) + (() if first else (prev,))
    return pl.pallas_call(
        lambda *refs: step_body(first, *refs),
        in_specs=[pl.BlockSpec(memory_space=pltpu.SMEM)] + [vmem] * (len(args) - 1),
        out_specs=vmem,
        out_shape=jax.ShapeDtypeStruct((ORB * HALF, CELLS), F32),
        compiler_params=LIMIT,
    )(*args)


def gram_body(*refs):
    pieces, out = refs[:-1], refs[-1]
    total = jnp.zeros((NVEC, 2 * NVEC), F32)
    for o in range(0, ORB, 2):
        rows = jnp.concatenate(
            [
                jnp.concatenate([p[(o + i) * HALF : (o + i + 1) * HALF, :] for p in pieces], axis=0)
                for i in range(2)
            ],
            axis=1,
        )
        high, low = split(rows)
        both = jnp.concatenate([high, low], axis=0)
        total = total + lax.dot_general(
            high, both, (((1,), (1,)), ((), ())), preferred_element_type=F32
        )
    cross = total[:, NVEC:]
    gram = total[:, :NVEC] + cross + jnp.transpose(cross)
    q = NVEC // 4
    out[: q, :] = jnp.concatenate(
        [gram[:q], gram[q : 2 * q, q:], gram[3 * q :, 3 * q :]], axis=1
    )
    row = gram[2 * q : 3 * q, 2 * q :]
    pad = jnp.zeros((q // 2, 2 * NVEC - 4 * q), F32)
    out[q:, :] = jnp.concatenate([row[: q // 2], row[q // 2 :], pad], axis=1)


def gram_of(pieces):
    return pl.pallas_call(
        gram_body,
        out_shape=jax.ShapeDtypeStruct((3 * NVEC // 8, 2 * NVEC), F32),
        compiler_params=LIMIT,
    )(*pieces)


def mix_body(factor, copies, *refs):
    pieces, out = refs[:-1], refs[-1]
    packed = jnp.sum(copies[...], axis=0)
    q = NVEC // 4
    row = lax.broadcasted_iota(jnp.int32, packed.shape, 0)
    at = lax.broadcasted_iota(jnp.int32, packed.shape, 1)
    upper = jnp.where((at < q) | ((at >= 4 * q) & (at < 5 * q)) | (at >= 7 * q), 1.0, 2.0)
    lower = jnp.where(at % (2 * q) < q, 1.0, 2.0)
    weighted = packed * packed * jnp.where(row < q, upper, lower)
    squares = jnp.sum(jnp.sum(weighted, axis=1, keepdims=True), axis=0, keepdims=True)
    frobenius = jnp.sqrt(squares)
    mine = packed[:q, :NVEC]
    rows = lax.broadcasted_iota(jnp.int32, mine.shape, 0)
    cols = lax.broadcasted_iota(jnp.int32, mine.shape, 1)
    eye = jnp.where(rows == cols, 1.0, 0.0).astype(F32)
    mixing = (1.5 * eye - 0.5 * mine / frobenius) * (factor / jnp.sqrt(frobenius))
    tall = jnp.concatenate([mixing] * 4, axis=0)
    wide = jnp.concatenate([tall] * 4, axis=1)
    rows = lax.broadcasted_iota(jnp.int32, wide.shape, 0) // (2 * HALF)
    cols = lax.broadcasted_iota(jnp.int32, wide.shape, 1) // NVEC
    wide = jnp.where(rows == cols, wide, 0.0)
    high, low = split(wide)
    high_lhs = high
    both_lhs = jnp.concatenate([high, low], axis=0)
    for group in range(ORB // 8):
        halves = []
        for side in range(2):
            at = group * 8 + side * 4
            halves.append(
                jnp.concatenate(
                    [
                        p[(at + i) * HALF : (at + i + 1) * HALF, :]
                        for i in range(4)
                        for p in pieces
                    ],
                    axis=0,
                )
            )
        data = jnp.concatenate(halves, axis=1)
        high, low = split(data)
        both = jnp.dot(both_lhs, high, preferred_element_type=F32)
        mixed = jnp.dot(high_lhs, low, preferred_element_type=F32)
        mixed = mixed + both[: 8 * HALF] + both[8 * HALF :]
        for side in range(2):
            at = (group * 8 + side * 4) * 2 * HALF
            out[at : at + 8 * HALF, :] = mixed[:, side * CELLS : (side + 1) * CELLS]


def mix(factor, copies, pieces):
    return pl.pallas_call(
        lambda *refs: mix_body(factor, *refs),
        out_shape=jax.ShapeDtypeStruct((ORB * 2 * HALF, CELLS), F32),
        compiler_params=LIMIT,
    )(copies, *pieces)


def shards(vectors, potential, hopping, center):
    cells = ("chip", "core")
    count = lax.axis_size("chip") * lax.axis_size("core")
    ring = lax.axis_size("vecs")
    outer = [(i, (i + 1) % count if i % 2 else (i - 1) % count) for i in range(count)]
    inner = [(0, 1), (1, 0)]
    near = [(i, i ^ 1) for i in range(ring)]
    other = [(i, i ^ 3) for i in range(ring)]
    pot = potential.reshape(ORB, CELLS)
    halves = [h.reshape(ORB * HALF, CELLS) for h in split_halves(vectors.reshape(ORB, -1, CELLS))]
    core = lax.axis_index("core")
    order = jnp.stack([2 * core, jnp.ones_like(core), 2 - 2 * core]).astype(jnp.int32)
    w = weights(order, hopping)
    prev = [None, None]
    cur = halves
    for step in range(STEPS):
        following = []
        for h in range(2):
            away = lax.ppermute(cur[h], cells, outer)
            beside = lax.ppermute(cur[h], "core", inner)
            following.append(apply_step(center, pot, w, cur[h], away, beside, prev[h]))
        prev, cur = cur, following
    a, b = cur
    a_near = lax.ppermute(a, "vecs", near)
    a_other = lax.ppermute(a, "vecs", other)
    a_far = lax.ppermute(a_other, "vecs", near)
    b_near = lax.ppermute(b, "vecs", near)
    b_other = lax.ppermute(b, "vecs", other)
    b_far = lax.ppermute(b_near, "vecs", other)
    pieces = (a, b, a_near, b_near, a_far, b_far, a_other, b_other)
    gram = gram_of(pieces)
    gram = gram + lax.ppermute(gram, "core", [(0, 1), (1, 0)])
    chips = lax.axis_size("chip")
    copies = lax.all_to_all(
        jnp.broadcast_to(gram, (chips, *gram.shape)), "chip", split_axis=0, concat_axis=0, tiled=True
    )
    factor = math.sqrt(float(count * CELLS))
    out = mix(factor, copies, pieces)
    return out.reshape(ORB, 1, 2 * HALF, CELLS)


def solution(mesh):
    cells, vecs = mesh.shape["cells"], mesh.shape["vecs"]
    fine = Mesh(mesh.devices.reshape(cells // 2, 2, vecs), ("chip", "core", "vecs"))
    both = ("chip", "core")
    placed = (P(None, both, "vecs", None), P(None, both, None), P(), P())
    return jax.shard_map(
        shards,
        mesh=fine,
        in_specs=placed,
        out_specs=P(None, both, "vecs", None),
        check_vma=False,
    )
```

```python
import math

import jax
import jax.numpy as jnp
from jax import lax
from jax.experimental import pallas as pl
from jax.experimental.pallas import tpu as pltpu
from jax.sharding import Mesh, PartitionSpec as P


ORB = 64
NVEC = 64
NY = 16
NZ = 8
CELLS = NY * NZ
STEPS = 4
HALF = 8
F32 = jnp.float32
BF16 = jnp.bfloat16


LIMIT = pltpu.CompilerParams(vmem_limit_bytes=8 * 1024 * 1024)


def split(x):
    high = x.astype(BF16)
    return high, (x - high.astype(F32)).astype(BF16)


def halves_body(vectors, *refs):
    copies = [
        pltpu.make_async_copy(vectors.at[:, h * HALF : (h + 1) * HALF], refs[h], refs[2 + h])
        for h in range(2)
    ]
    for copy in copies:
        copy.start()
    for copy in copies:
        copy.wait()


def split_halves(vectors):
    vmem = pl.BlockSpec(memory_space=pltpu.VMEM)
    return pl.pallas_call(
        halves_body,
        in_specs=[pl.BlockSpec(memory_space=pl.ANY)],
        out_specs=[vmem, vmem],
        out_shape=[jax.ShapeDtypeStruct((ORB, HALF, CELLS), F32)] * 2,
        scratch_shapes=[pltpu.SemaphoreType.DMA, pltpu.SemaphoreType.DMA],
        compiler_params=LIMIT,
    )(vectors)


def weights_body(order, hop, out):
    for iz in range(3):
        parts = []
        for iy in range(3):
            for ix in range(3):
                d = 9 * order[ix] + 3 * iy + iz
                parts.append(0.5 * (hop[d] + jnp.transpose(hop[26 - d])))
        high, low = split(jnp.concatenate(parts, axis=1))
        high = high.astype(F32)
        whole = jnp.concatenate([high, high, low.astype(F32)], axis=1)
        out[iz * ORB : (iz + 1) * ORB, :] = whole.astype(BF16)


def weights(order, hopping):
    return pl.pallas_call(
        weights_body,
        in_specs=[pl.BlockSpec(memory_space=pltpu.SMEM), pl.BlockSpec(memory_space=pltpu.VMEM)],
        out_shape=jax.ShapeDtypeStruct((3 * ORB, 27 * ORB), BF16),
        compiler_params=LIMIT,
    )(order, hopping)


def step_body(first, *refs):
    if first:
        center, pot, w, cur, left, right, out = refs
    else:
        center, pot, w, cur, left, right, prev, out = refs
    onsite = pot[...] - center[0]
    lane = lax.broadcasted_iota(jnp.int32, (ORB, CELLS), 1) % NZ
    for pair in range(HALF // 2):
        rows = [pl.ds(2 * pair + i, ORB, stride=HALF) for i in range(2)]
        own = [cur[r, :] for r in rows]
        columns = []
        for i in range(2):
            here = jnp.concatenate([left[rows[i], :], own[i], right[rows[i], :]], axis=0)
            below, above = pltpu.roll(here, NZ, 1), pltpu.roll(here, CELLS - NZ, 1)
            columns.append(jnp.concatenate([below, here, above], axis=0))
        high, low = split(jnp.concatenate(columns, axis=1))
        stacked = jnp.concatenate([high, low, high], axis=0)
        product = jnp.dot(w[...], stacked, preferred_element_type=F32)
        for i in range(2):
            below, here, above = (
                product[iz * ORB : (iz + 1) * ORB, i * CELLS : (i + 1) * CELLS] for iz in range(3)
            )
            below = jnp.where(
                lane == 0, pltpu.roll(below, CELLS - NZ + 1, 1), pltpu.roll(below, 1, 1)
            )
            above = jnp.where(
                lane == NZ - 1, pltpu.roll(above, NZ - 1, 1), pltpu.roll(above, CELLS - 1, 1)
            )
            total = onsite * own[i] + here + below + above
            if not first:
                total = 2.0 * total - prev[rows[i], :]
            out[rows[i], :] = total


def apply_step(center, pot, w, cur, left, right, prev=None):
    first = prev is None
    vmem = pl.BlockSpec(memory_space=pltpu.VMEM)
    args = (center, pot, w, cur, left, right) + (() if first else (prev,))
    return pl.pallas_call(
        lambda *refs: step_body(first, *refs),
        in_specs=[pl.BlockSpec(memory_space=pltpu.SMEM)] + [vmem] * (len(args) - 1),
        out_specs=vmem,
        out_shape=jax.ShapeDtypeStruct((ORB * HALF, CELLS), F32),
        compiler_params=LIMIT,
    )(*args)


def changed_over(x, flag, axis):
    quarters = jnp.split(x, 4, axis=axis)
    return jnp.where(flag[0] == 1, jnp.concatenate([quarters[i] for i in (0, 3, 2, 1)], axis), x)


def gram_body(flag, *refs):
    pieces, out = refs[:-1], refs[-1]
    total = jnp.zeros((NVEC, 2 * NVEC), F32)
    for o in range(0, ORB, 2):
        rows = jnp.concatenate(
            [
                jnp.concatenate([p[(o + i) * HALF : (o + i + 1) * HALF, :] for p in pieces], axis=0)
                for i in range(2)
            ],
            axis=1,
        )
        high, low = split(rows)
        both = jnp.concatenate([high, low], axis=0)
        total = total + lax.dot_general(
            high, both, (((1,), (1,)), ((), ())), preferred_element_type=F32
        )
    cross = total[:, NVEC:]
    gram = total[:, :NVEC] + cross + jnp.transpose(cross)
    gram = changed_over(changed_over(gram, flag, 0), flag, 1)
    q = NVEC // 4
    out[: q, :] = jnp.concatenate(
        [gram[:q], gram[q : 2 * q, q:], gram[3 * q :, 3 * q :]], axis=1
    )
    row = gram[2 * q : 3 * q, 2 * q :]
    pad = jnp.zeros((q // 2, 2 * NVEC - 4 * q), F32)
    out[q:, :] = jnp.concatenate([row[: q // 2], row[q // 2 :], pad], axis=1)


def gram_of(flag, pieces):
    vmem = pl.BlockSpec(memory_space=pltpu.VMEM)
    return pl.pallas_call(
        gram_body,
        in_specs=[pl.BlockSpec(memory_space=pltpu.SMEM)] + [vmem] * len(pieces),
        out_shape=jax.ShapeDtypeStruct((3 * NVEC // 8, 2 * NVEC), F32),
        compiler_params=LIMIT,
    )(flag, *pieces)


def mix_body(factor, flag, copies, *refs):
    pieces, out = refs[:-1], refs[-1]
    packed = jnp.sum(copies[...], axis=0)
    q = NVEC // 4
    row = lax.broadcasted_iota(jnp.int32, packed.shape, 0)
    at = lax.broadcasted_iota(jnp.int32, packed.shape, 1)
    upper = jnp.where((at < q) | ((at >= 4 * q) & (at < 5 * q)) | (at >= 7 * q), 1.0, 2.0)
    lower = jnp.where(at % (2 * q) < q, 1.0, 2.0)
    weighted = packed * packed * jnp.where(row < q, upper, lower)
    squares = jnp.sum(jnp.sum(weighted, axis=1, keepdims=True), axis=0, keepdims=True)
    frobenius = jnp.sqrt(squares)
    mine = packed[:q, :NVEC]
    rows = lax.broadcasted_iota(jnp.int32, mine.shape, 0)
    cols = lax.broadcasted_iota(jnp.int32, mine.shape, 1)
    eye = jnp.where(rows == cols, 1.0, 0.0).astype(F32)
    mixing = (1.5 * eye - 0.5 * mine / frobenius) * (factor / jnp.sqrt(frobenius))
    mixing = changed_over(mixing, flag, 1)
    tall = jnp.concatenate([mixing] * 4, axis=0)
    wide = jnp.concatenate([tall] * 4, axis=1)
    rows = lax.broadcasted_iota(jnp.int32, wide.shape, 0) // (2 * HALF)
    cols = lax.broadcasted_iota(jnp.int32, wide.shape, 1) // NVEC
    wide = jnp.where(rows == cols, wide, 0.0)
    high, low = split(wide)
    high_lhs = high
    both_lhs = jnp.concatenate([high, low], axis=0)
    for group in range(ORB // 8):
        halves = []
        for side in range(2):
            at = group * 8 + side * 4
            halves.append(
                jnp.concatenate(
                    [
                        p[(at + i) * HALF : (at + i + 1) * HALF, :]
                        for i in range(4)
                        for p in pieces
                    ],
                    axis=0,
                )
            )
        data = jnp.concatenate(halves, axis=1)
        high, low = split(data)
        both = jnp.dot(both_lhs, high, preferred_element_type=F32)
        mixed = jnp.dot(high_lhs, low, preferred_element_type=F32)
        mixed = mixed + both[: 8 * HALF] + both[8 * HALF :]
        for side in range(2):
            at = (group * 8 + side * 4) * 2 * HALF
            out[at : at + 8 * HALF, :] = mixed[:, side * CELLS : (side + 1) * CELLS]


def mix(factor, flag, copies, pieces):
    vmem = pl.BlockSpec(memory_space=pltpu.VMEM)
    return pl.pallas_call(
        lambda *refs: mix_body(factor, *refs),
        in_specs=[pl.BlockSpec(memory_space=pltpu.SMEM)] + [vmem] * (1 + len(pieces)),
        out_shape=jax.ShapeDtypeStruct((ORB * 2 * HALF, CELLS), F32),
        compiler_params=LIMIT,
    )(flag, copies, *pieces)


def filtered(vectors, potential, hopping, center):
    cells = ("chip", "core")
    count = lax.axis_size("chip") * lax.axis_size("core")
    ring = lax.axis_size("vecs")
    outer = [(i, (i + 1) % count if i % 2 else (i - 1) % count) for i in range(count)]
    inner = [(0, 1), (1, 0)]
    flips = ((1, 3), (3, 1))
    early, late = (
        [(k * ring + i, k * ring + (i ^ flips[k][turn])) for k in range(2) for i in range(ring)]
        for turn in range(2)
    )
    pot = potential.reshape(ORB, CELLS)
    halves = [h.reshape(ORB * HALF, CELLS) for h in split_halves(vectors.reshape(ORB, -1, CELLS))]
    core = lax.axis_index("core")
    order = jnp.stack([2 * core, jnp.ones_like(core), 2 - 2 * core]).astype(jnp.int32)
    w = weights(order, hopping)
    prev = [None, None]
    cur = halves
    for _ in range(STEPS):
        following = []
        for h in range(2):
            away = lax.ppermute(cur[h], cells, outer)
            beside = lax.ppermute(cur[h], "core", inner)
            following.append(apply_step(center, pot, w, cur[h], away, beside, prev[h]))
        prev, cur = cur, following
    a, b = cur
    planes = ("core", "vecs")
    a_early = lax.ppermute(a, planes, early)
    a_late = lax.ppermute(a, planes, late)
    b_early = lax.ppermute(b, planes, early)
    b_late = lax.ppermute(b, planes, late)
    a_far = lax.ppermute(a_early, planes, late)
    b_far = lax.ppermute(b_early, planes, late)
    pieces = (a, b, a_early, b_early, a_far, b_far, a_late, b_late)
    flag = core.reshape(1).astype(jnp.int32)
    gram = gram_of(flag, pieces)
    gram = gram + lax.ppermute(gram, "core", [(0, 1), (1, 0)])
    chips = lax.axis_size("chip")
    copies = lax.all_to_all(
        jnp.broadcast_to(gram, (chips, *gram.shape)), "chip", split_axis=0, concat_axis=0, tiled=True
    )
    factor = math.sqrt(float(count * CELLS))
    out = mix(factor, flag, copies, pieces)
    return out.reshape(ORB, 1, 2 * HALF, CELLS)


def solution(mesh):
    cells, vecs = mesh.shape["cells"], mesh.shape["vecs"]
    fine = Mesh(mesh.devices.reshape(cells // 2, 2, vecs), ("chip", "core", "vecs"))
    both = ("chip", "core")
    placed = (P(None, both, "vecs", None), P(None, both, None), P(), P())
    return jax.shard_map(
        filtered,
        mesh=fine,
        in_specs=placed,
        out_specs=P(None, both, "vecs", None),
        check_vma=False,
    )
```

```python
import math

import jax
import jax.numpy as jnp
from jax import lax
from jax.experimental import pallas as pl
from jax.experimental.pallas import tpu as pltpu
from jax.sharding import Mesh, PartitionSpec as P


ORB = 64
NVEC = 64
NY = 16
NZ = 8
CELLS = NY * NZ
STEPS = 4
HALF = 8
F32 = jnp.float32
BF16 = jnp.bfloat16


LIMIT = pltpu.CompilerParams(vmem_limit_bytes=8 * 1024 * 1024)


def split(x):
    high = x.astype(BF16)
    return high, (x - high.astype(F32)).astype(BF16)


def halves_body(vectors, *refs):
    copies = [
        pltpu.make_async_copy(vectors.at[:, h * HALF : (h + 1) * HALF], refs[h], refs[2 + h])
        for h in range(2)
    ]
    for copy in copies:
        copy.start()
    for copy in copies:
        copy.wait()


def split_halves(vectors):
    vmem = pl.BlockSpec(memory_space=pltpu.VMEM)
    return pl.pallas_call(
        halves_body,
        in_specs=[pl.BlockSpec(memory_space=pl.ANY)],
        out_specs=[vmem, vmem],
        out_shape=[jax.ShapeDtypeStruct((ORB, HALF, CELLS), F32)] * 2,
        scratch_shapes=[pltpu.SemaphoreType.DMA, pltpu.SemaphoreType.DMA],
        compiler_params=LIMIT,
    )(vectors)


def weights_body(order, hop, out):
    for iz in range(3):
        parts = []
        for iy in range(3):
            for ix in range(3):
                d = 9 * order[ix] + 3 * iy + iz
                parts.append(0.5 * (hop[d] + jnp.transpose(hop[26 - d])))
        high, low = split(jnp.concatenate(parts, axis=1))
        high = high.astype(F32)
        whole = jnp.concatenate([high, high, low.astype(F32)], axis=1)
        out[iz * ORB : (iz + 1) * ORB, :] = whole.astype(BF16)


def weights(order, hopping):
    return pl.pallas_call(
        weights_body,
        in_specs=[pl.BlockSpec(memory_space=pltpu.SMEM), pl.BlockSpec(memory_space=pltpu.VMEM)],
        out_shape=jax.ShapeDtypeStruct((3 * ORB, 27 * ORB), BF16),
        compiler_params=LIMIT,
    )(order, hopping)


def step_body(first, *refs):
    if first:
        center, pot, w, cur, left, right, out = refs
    else:
        center, pot, w, cur, left, right, prev, out = refs
    onsite = pot[...] - center[0]
    lane = lax.broadcasted_iota(jnp.int32, (ORB, CELLS), 1) % NZ
    rows = [pl.ds(i, ORB, stride=HALF) for i in range(HALF)]
    columns = []
    for r in rows:
        here = jnp.concatenate([left[r, :], cur[r, :], right[r, :]], axis=0)
        below, above = pltpu.roll(here, NZ, 1), pltpu.roll(here, CELLS - NZ, 1)
        columns.append(jnp.concatenate([below, here, above], axis=0))
    high, low = split(jnp.concatenate(columns, axis=1))
    stacked = jnp.concatenate([high, low, high], axis=0)
    product = jnp.dot(w[...], stacked, preferred_element_type=F32)
    for i, r in enumerate(rows):
        below, here, above = (
            product[iz * ORB : (iz + 1) * ORB, i * CELLS : (i + 1) * CELLS] for iz in range(3)
        )
        below = jnp.where(lane == 0, pltpu.roll(below, CELLS - NZ + 1, 1), pltpu.roll(below, 1, 1))
        above = jnp.where(
            lane == NZ - 1, pltpu.roll(above, NZ - 1, 1), pltpu.roll(above, CELLS - 1, 1)
        )
        total = onsite * cur[r, :] + here + below + above
        if not first:
            total = 2.0 * total - prev[r, :]
        out[r, :] = total


def apply_step(center, pot, w, cur, left, right, prev=None):
    first = prev is None
    vmem = pl.BlockSpec(memory_space=pltpu.VMEM)
    args = (center, pot, w, cur, left, right) + (() if first else (prev,))
    return pl.pallas_call(
        lambda *refs: step_body(first, *refs),
        in_specs=[pl.BlockSpec(memory_space=pltpu.SMEM)] + [vmem] * (len(args) - 1),
        out_specs=vmem,
        out_shape=jax.ShapeDtypeStruct((ORB * HALF, CELLS), F32),
        compiler_params=LIMIT,
    )(*args)


def changed_over(x, flag, axis):
    quarters = jnp.split(x, 4, axis=axis)
    return jnp.where(flag[0] == 1, jnp.concatenate([quarters[i] for i in (0, 3, 2, 1)], axis), x)


def gram_body(flag, *refs):
    pieces, out = refs[:-1], refs[-1]
    total = jnp.zeros((2 * NVEC, NVEC), F32)
    for o in range(0, ORB, 2):
        rows = jnp.concatenate(
            [
                jnp.concatenate([p[(o + i) * HALF : (o + i + 1) * HALF, :] for p in pieces], axis=0)
                for i in range(2)
            ],
            axis=1,
        )
        high, low = split(rows)
        both = jnp.concatenate([high, low], axis=0)
        total = total + lax.dot_general(
            both, high, (((1,), (1,)), ((), ())), preferred_element_type=F32
        )
    cross = total[NVEC:]
    gram = total[:NVEC] + cross + jnp.transpose(cross)
    gram = changed_over(changed_over(gram, flag, 0), flag, 1)
    q = NVEC // 4
    out[: q, :] = jnp.concatenate(
        [gram[:q], gram[q : 2 * q, q:], gram[3 * q :, 3 * q :]], axis=1
    )
    row = gram[2 * q : 3 * q, 2 * q :]
    pad = jnp.zeros((q // 2, 2 * NVEC - 4 * q), F32)
    out[q:, :] = jnp.concatenate([row[: q // 2], row[q // 2 :], pad], axis=1)


def gram_of(flag, pieces):
    vmem = pl.BlockSpec(memory_space=pltpu.VMEM)
    return pl.pallas_call(
        gram_body,
        in_specs=[pl.BlockSpec(memory_space=pltpu.SMEM)] + [vmem] * len(pieces),
        out_shape=jax.ShapeDtypeStruct((3 * NVEC // 8, 2 * NVEC), F32),
        compiler_params=LIMIT,
    )(flag, *pieces)


def mix_body(factor, flag, copies, *refs):
    pieces, result, out, semaphores = refs[:-3], refs[-3], refs[-2], refs[-1]
    transfers = []
    packed = jnp.sum(copies[...], axis=0)
    q = NVEC // 4
    row = lax.broadcasted_iota(jnp.int32, packed.shape, 0)
    at = lax.broadcasted_iota(jnp.int32, packed.shape, 1)
    upper = jnp.where((at < q) | ((at >= 4 * q) & (at < 5 * q)) | (at >= 7 * q), 1.0, 2.0)
    lower = jnp.where(at % (2 * q) < q, 1.0, 2.0)
    weighted = packed * packed * jnp.where(row < q, upper, lower)
    squares = jnp.sum(jnp.sum(weighted, axis=1, keepdims=True), axis=0, keepdims=True)
    frobenius = jnp.sqrt(squares)
    mine = packed[:q, :NVEC]
    rows = lax.broadcasted_iota(jnp.int32, mine.shape, 0)
    cols = lax.broadcasted_iota(jnp.int32, mine.shape, 1)
    eye = jnp.where(rows == cols, 1.0, 0.0).astype(F32)
    mixing = (1.5 * eye - 0.5 * mine / frobenius) * (factor / jnp.sqrt(frobenius))
    mixing = changed_over(mixing, flag, 1)
    tall = jnp.concatenate([mixing] * 4, axis=0)
    wide = jnp.concatenate([tall] * 4, axis=1)
    rows = lax.broadcasted_iota(jnp.int32, wide.shape, 0) // (2 * HALF)
    cols = lax.broadcasted_iota(jnp.int32, wide.shape, 1) // NVEC
    wide = jnp.where(rows == cols, wide, 0.0)
    high, low = split(wide)
    high_lhs = high
    both_lhs = jnp.concatenate([high, low], axis=0)
    for group in range(ORB // 8):
        halves = []
        for side in range(2):
            at = group * 8 + side * 4
            halves.append(
                jnp.concatenate(
                    [
                        p[(at + i) * HALF : (at + i + 1) * HALF, :]
                        for i in range(4)
                        for p in pieces
                    ],
                    axis=0,
                )
            )
        data = jnp.concatenate(halves, axis=1)
        high, low = split(data)
        both = jnp.dot(both_lhs, high, preferred_element_type=F32)
        mixed = jnp.dot(high_lhs, low, preferred_element_type=F32)
        mixed = mixed + both[: 8 * HALF] + both[8 * HALF :]
        for side in range(2):
            at = (group * 8 + side * 4) * 2 * HALF
            out[at : at + 8 * HALF, :] = mixed[:, side * CELLS : (side + 1) * CELLS]
        done = pl.ds(group * 16 * HALF, 16 * HALF)
        transfers.append(
            pltpu.make_async_copy(out.at[done], result.at[done], semaphores.at[group])
        )
        transfers[-1].start()
    for transfer in transfers:
        transfer.wait()


def mix(factor, flag, copies, pieces):
    vmem = pl.BlockSpec(memory_space=pltpu.VMEM)
    return pl.pallas_call(
        lambda *refs: mix_body(factor, *refs),
        in_specs=[pl.BlockSpec(memory_space=pltpu.SMEM)] + [vmem] * (1 + len(pieces)),
        out_specs=pl.BlockSpec(memory_space=pltpu.HBM),
        out_shape=jax.ShapeDtypeStruct((ORB * 2 * HALF, CELLS), F32),
        scratch_shapes=[
            pltpu.VMEM((ORB * 2 * HALF, CELLS), F32),
            pltpu.SemaphoreType.DMA((ORB // 8,)),
        ],
        compiler_params=LIMIT,
    )(flag, copies, *pieces)


def filtered(vectors, potential, hopping, center):
    cells = ("chip", "core")
    count = lax.axis_size("chip") * lax.axis_size("core")
    ring = lax.axis_size("vecs")
    outer = [(i, (i + 1) % count if i % 2 else (i - 1) % count) for i in range(count)]
    inner = [(0, 1), (1, 0)]
    flips = ((1, 3), (3, 1))
    early, late = (
        [(k * ring + i, k * ring + (i ^ flips[k][turn])) for k in range(2) for i in range(ring)]
        for turn in range(2)
    )
    pot = potential.reshape(ORB, CELLS)
    halves = [h.reshape(ORB * HALF, CELLS) for h in split_halves(vectors.reshape(ORB, -1, CELLS))]
    core = lax.axis_index("core")
    order = jnp.stack([2 * core, jnp.ones_like(core), 2 - 2 * core]).astype(jnp.int32)
    w = weights(order, hopping)
    prev = [None, None]
    cur = halves
    for _ in range(STEPS):
        following = []
        for h in range(2):
            away = lax.ppermute(cur[h], cells, outer)
            beside = lax.ppermute(cur[h], "core", inner)
            following.append(apply_step(center, pot, w, cur[h], away, beside, prev[h]))
        prev, cur = cur, following
    a, b = cur
    planes = ("core", "vecs")
    a_early = lax.ppermute(a, planes, early)
    a_late = lax.ppermute(a, planes, late)
    b_early = lax.ppermute(b, planes, early)
    b_late = lax.ppermute(b, planes, late)
    a_far = lax.ppermute(a_early, planes, late)
    b_far = lax.ppermute(b_early, planes, late)
    pieces = (a, b, a_early, b_early, a_far, b_far, a_late, b_late)
    flag = core.reshape(1).astype(jnp.int32)
    gram = gram_of(flag, pieces)
    gram = gram + lax.ppermute(gram, "core", [(0, 1), (1, 0)])
    chips = lax.axis_size("chip")
    copies = lax.all_to_all(
        jnp.broadcast_to(gram, (chips, *gram.shape)), "chip", split_axis=0, concat_axis=0, tiled=True
    )
    factor = math.sqrt(float(count * CELLS))
    out = mix(factor, flag, copies, pieces)
    return out.reshape(ORB, 1, 2 * HALF, CELLS)


def solution(mesh):
    cells, vecs = mesh.shape["cells"], mesh.shape["vecs"]
    fine = Mesh(mesh.devices.reshape(cells // 2, 2, vecs), ("chip", "core", "vecs"))
    both = ("chip", "core")
    placed = (P(None, both, "vecs", None), P(None, both, None), P(), P())
    return jax.shard_map(
        filtered,
        mesh=fine,
        in_specs=placed,
        out_specs=P(None, both, "vecs", None),
        check_vma=False,
    )
```

```python
import math

import jax
import jax.numpy as jnp
from jax import lax
from jax.experimental import pallas as pl
from jax.experimental.pallas import tpu as pltpu
from jax.sharding import Mesh, PartitionSpec as P


ORB = 64
NVEC = 64
NY = 16
NZ = 8
CELLS = NY * NZ
STEPS = 4
HALF = 8
F32 = jnp.float32
BF16 = jnp.bfloat16


LIMIT = pltpu.CompilerParams(vmem_limit_bytes=8 * 1024 * 1024)


def split(x):
    high = x.astype(BF16)
    return high, (x - high.astype(F32)).astype(BF16)


def halves_body(vectors, *refs):
    copies = [
        pltpu.make_async_copy(vectors.at[:, h * HALF : (h + 1) * HALF], refs[h], refs[2 + h])
        for h in range(2)
    ]
    for copy in copies:
        copy.start()
    for copy in copies:
        copy.wait()


def split_halves(vectors):
    vmem = pl.BlockSpec(memory_space=pltpu.VMEM)
    return pl.pallas_call(
        halves_body,
        in_specs=[pl.BlockSpec(memory_space=pl.ANY)],
        out_specs=[vmem, vmem],
        out_shape=[jax.ShapeDtypeStruct((ORB, HALF, CELLS), F32)] * 2,
        scratch_shapes=[pltpu.SemaphoreType.DMA, pltpu.SemaphoreType.DMA],
        compiler_params=LIMIT,
    )(vectors)


def weights_body(order, hop, out):
    for iz in range(3):
        parts = []
        for iy in range(3):
            for ix in range(3):
                d = 9 * order[ix] + 3 * iy + iz
                parts.append(0.5 * (hop[d] + jnp.transpose(hop[26 - d])))
        high, low = split(jnp.concatenate(parts, axis=1))
        high = high.astype(F32)
        whole = jnp.concatenate([high, high, low.astype(F32)], axis=1)
        out[iz * ORB : (iz + 1) * ORB, :] = whole.astype(BF16)


def weights(order, hopping):
    return pl.pallas_call(
        weights_body,
        in_specs=[pl.BlockSpec(memory_space=pltpu.SMEM), pl.BlockSpec(memory_space=pltpu.VMEM)],
        out_shape=jax.ShapeDtypeStruct((3 * ORB, 27 * ORB), BF16),
        compiler_params=LIMIT,
    )(order, hopping)


def step_body(first, *refs):
    if first:
        center, pot, w, cur, left, right, out = refs
    else:
        center, pot, w, cur, left, right, prev, out = refs
    onsite = pot[...] - center[0]
    lane = lax.broadcasted_iota(jnp.int32, (ORB, CELLS), 1) % NZ
    rows = [pl.ds(i, ORB, stride=HALF) for i in range(HALF)]
    columns = []
    for r in rows:
        here = jnp.concatenate([left[r, :], cur[r, :], right[r, :]], axis=0)
        below, above = pltpu.roll(here, NZ, 1), pltpu.roll(here, CELLS - NZ, 1)
        columns.append(jnp.concatenate([below, here, above], axis=0))
    high, low = split(jnp.concatenate(columns, axis=1))
    stacked = jnp.concatenate([high, low, high], axis=0)
    product = jnp.dot(w[...], stacked, preferred_element_type=F32)
    for i, r in enumerate(rows):
        below, here, above = (
            product[iz * ORB : (iz + 1) * ORB, i * CELLS : (i + 1) * CELLS] for iz in range(3)
        )
        below = jnp.where(lane == 0, pltpu.roll(below, CELLS - NZ + 1, 1), pltpu.roll(below, 1, 1))
        above = jnp.where(
            lane == NZ - 1, pltpu.roll(above, NZ - 1, 1), pltpu.roll(above, CELLS - 1, 1)
        )
        total = onsite * cur[r, :] + here + below + above
        if not first:
            total = 2.0 * total - prev[r, :]
        out[r, :] = total


def apply_step(center, pot, w, cur, left, right, prev=None):
    first = prev is None
    vmem = pl.BlockSpec(memory_space=pltpu.VMEM)
    args = (center, pot, w, cur, left, right) + (() if first else (prev,))
    return pl.pallas_call(
        lambda *refs: step_body(first, *refs),
        in_specs=[pl.BlockSpec(memory_space=pltpu.SMEM)] + [vmem] * (len(args) - 1),
        out_specs=vmem,
        out_shape=jax.ShapeDtypeStruct((ORB * HALF, CELLS), F32),
        compiler_params=LIMIT,
    )(*args)


def changed_over(x, flag, axis):
    quarters = jnp.split(x, 4, axis=axis)
    return jnp.where(flag[0] == 1, jnp.concatenate([quarters[i] for i in (0, 3, 2, 1)], axis), x)


def gram_body(flag, *refs):
    pieces, out = refs[:-1], refs[-1]
    total = jnp.zeros((2 * NVEC, NVEC), F32)
    for o in range(0, ORB, 2):
        rows = jnp.concatenate(
            [
                jnp.concatenate([p[(o + i) * HALF : (o + i + 1) * HALF, :] for p in pieces], axis=0)
                for i in range(2)
            ],
            axis=1,
        )
        high, low = split(rows)
        both = jnp.concatenate([high, low], axis=0)
        total = total + lax.dot_general(
            both, high, (((1,), (1,)), ((), ())), preferred_element_type=F32
        )
    cross = total[NVEC:]
    gram = total[:NVEC] + cross + jnp.transpose(cross)
    gram = changed_over(changed_over(gram, flag, 0), flag, 1)
    q = NVEC // 4
    out[: q, :] = jnp.concatenate(
        [gram[:q], gram[q : 2 * q, q:], gram[3 * q :, 3 * q :]], axis=1
    )
    row = gram[2 * q : 3 * q, 2 * q :]
    pad = jnp.zeros((q // 2, 2 * NVEC - 4 * q), F32)
    out[q:, :] = jnp.concatenate([row[: q // 2], row[q // 2 :], pad], axis=1)


def gram_of(flag, pieces):
    vmem = pl.BlockSpec(memory_space=pltpu.VMEM)
    return pl.pallas_call(
        gram_body,
        in_specs=[pl.BlockSpec(memory_space=pltpu.SMEM)] + [vmem] * len(pieces),
        out_shape=jax.ShapeDtypeStruct((3 * NVEC // 8, 2 * NVEC), F32),
        compiler_params=LIMIT,
    )(flag, *pieces)


def mix_body(factor, flag, copies, *refs):
    pieces, result, out, semaphores = refs[:-3], refs[-3], refs[-2], refs[-1]
    transfers = []
    packed = jnp.sum(copies[...], axis=0)
    q = NVEC // 4
    row = lax.broadcasted_iota(jnp.int32, packed.shape, 0)
    at = lax.broadcasted_iota(jnp.int32, packed.shape, 1)
    upper = jnp.where((at < q) | ((at >= 4 * q) & (at < 5 * q)) | (at >= 7 * q), 1.0, 2.0)
    lower = jnp.where(at % (2 * q) < q, 1.0, 2.0)
    weighted = packed * packed * jnp.where(row < q, upper, lower)
    squares = jnp.sum(jnp.sum(weighted, axis=1, keepdims=True), axis=0, keepdims=True)
    frobenius = jnp.sqrt(squares)
    mine = packed[:q, :NVEC]
    rows = lax.broadcasted_iota(jnp.int32, mine.shape, 0)
    cols = lax.broadcasted_iota(jnp.int32, mine.shape, 1)
    eye = jnp.where(rows == cols, 1.0, 0.0).astype(F32)
    mixing = (1.5 * eye - 0.5 * mine / frobenius) * (factor / jnp.sqrt(frobenius))
    mixing = changed_over(mixing, flag, 1)
    tall = jnp.concatenate([mixing] * 4, axis=0)
    wide = jnp.concatenate([tall] * 4, axis=1)
    rows = lax.broadcasted_iota(jnp.int32, wide.shape, 0) // (2 * HALF)
    cols = lax.broadcasted_iota(jnp.int32, wide.shape, 1) // NVEC
    wide = jnp.where(rows == cols, wide, 0.0)
    high, low = split(wide)
    high_lhs = high
    both_lhs = jnp.concatenate([high, low], axis=0)
    for group in range(ORB // 8):
        halves = []
        for side in range(2):
            at = group * 8 + side * 4
            halves.append(
                jnp.concatenate(
                    [
                        p[(at + i) * HALF : (at + i + 1) * HALF, :]
                        for i in range(4)
                        for p in pieces
                    ],
                    axis=0,
                )
            )
        data = jnp.concatenate(halves, axis=1)
        high, low = split(data)
        both = jnp.dot(both_lhs, high, preferred_element_type=F32)
        mixed = jnp.dot(high_lhs, low, preferred_element_type=F32)
        mixed = mixed + both[: 8 * HALF] + both[8 * HALF :]
        for side in range(2):
            at = (group * 8 + side * 4) * 2 * HALF
            out[at : at + 8 * HALF, :] = mixed[:, side * CELLS : (side + 1) * CELLS]
        done = pl.ds(group * 16 * HALF, 16 * HALF)
        transfers.append(
            pltpu.make_async_copy(out.at[done], result.at[done], semaphores.at[group])
        )
        transfers[-1].start()
    for transfer in transfers:
        transfer.wait()


def mix(factor, flag, copies, pieces):
    vmem = pl.BlockSpec(memory_space=pltpu.VMEM)
    return pl.pallas_call(
        lambda *refs: mix_body(factor, *refs),
        in_specs=[pl.BlockSpec(memory_space=pltpu.SMEM)] + [vmem] * (1 + len(pieces)),
        out_specs=pl.BlockSpec(memory_space=pltpu.HBM),
        out_shape=jax.ShapeDtypeStruct((ORB * 2 * HALF, CELLS), F32),
        scratch_shapes=[
            pltpu.VMEM((ORB * 2 * HALF, CELLS), F32),
            pltpu.SemaphoreType.DMA((ORB // 8,)),
        ],
        compiler_params=LIMIT,
    )(flag, copies, *pieces)


def filtered(vectors, potential, hopping, center):
    cells = ("chip", "core")
    count = lax.axis_size("chip") * lax.axis_size("core")
    ring = lax.axis_size("vecs")
    outer = [(i, (i + 1) % count if i % 2 else (i - 1) % count) for i in range(count)]
    inner = [(0, 1), (1, 0)]
    flips = ((3, 1), (1, 3))
    early, late = (
        [(k * ring + i, k * ring + (i ^ flips[k][turn])) for k in range(2) for i in range(ring)]
        for turn in range(2)
    )
    pot = potential.reshape(ORB, CELLS)
    halves = [h.reshape(ORB * HALF, CELLS) for h in split_halves(vectors.reshape(ORB, -1, CELLS))]
    core = lax.axis_index("core")
    order = jnp.stack([2 * core, jnp.ones_like(core), 2 - 2 * core]).astype(jnp.int32)
    w = weights(order, hopping)
    prev = [None, None]
    cur = halves
    for _ in range(STEPS):
        following = []
        for h in range(2):
            away = lax.ppermute(cur[h], cells, outer)
            beside = lax.ppermute(cur[h], "core", inner)
            following.append(apply_step(center, pot, w, cur[h], away, beside, prev[h]))
        prev, cur = cur, following
    a, b = cur
    planes = ("core", "vecs")
    a_early = lax.ppermute(a, planes, early)
    a_late = lax.ppermute(a, planes, late)
    b_early = lax.ppermute(b, planes, early)
    b_late = lax.ppermute(b, planes, late)
    a_far = lax.ppermute(a_early, planes, late)
    b_far = lax.ppermute(b_early, planes, late)
    pieces = (a, b, a_early, b_early, a_far, b_far, a_late, b_late)
    flag = core.reshape(1).astype(jnp.int32)
    gram = gram_of(flag, pieces)
    copies = lax.all_to_all(
        jnp.broadcast_to(gram, (count, *gram.shape)), cells, split_axis=0, concat_axis=0, tiled=True
    )
    factor = math.sqrt(float(count * CELLS))
    out = mix(factor, flag, copies, pieces)
    return out.reshape(ORB, 1, 2 * HALF, CELLS)


def solution(mesh):
    cells, vecs = mesh.shape["cells"], mesh.shape["vecs"]
    fine = Mesh(mesh.devices.reshape(cells // 2, 2, vecs), ("chip", "core", "vecs"))
    both = ("chip", "core")
    placed = (P(None, both, "vecs", None), P(None, both, None), P(), P())
    return jax.shard_map(
        filtered,
        mesh=fine,
        in_specs=placed,
        out_specs=P(None, both, "vecs", None),
        check_vma=False,
    )
```
